256 devices in a mesh: fsdp: 4 (over x), tensor: 4 (over y_lo, core), dp: 16 (over y_hi, z).
Axes of the slice: x: 4, y: 4 (y_hi: 2, y_lo: 2; y = y_hi * 2 + y_lo), z: 8, core: 2. Of those that a mesh axis runs over, the one named last changes fastest.
Arguments:
- tokens: bfloat16 [1024, 8192], P('fsdp', 'dp'), may hold values from -6 to 6
- cotangent: bfloat16 [1024, 8192], P('fsdp', 'dp'), may hold values from -6 to 6
- gate_weight: bfloat16 [8192, 28672], P('fsdp', ('tensor', 'dp')), may hold values from -0.0625 to 0.0625
- up_weight: bfloat16 [8192, 28672], P('fsdp', ('tensor', 'dp')), may hold values from -0.0625 to 0.0625
- down_weight: bfloat16 [28672, 8192], P(('tensor', 'dp'), 'fsdp'), may hold values from -0.03125 to 0.03125
- model_projection: bfloat16 [64, 8192], replicated, may hold values from -0.0625 to 0.0625
- hidden_projection: bfloat16 [64, 28672], P(None, ('tensor', 'dp')), may hold values from -0.03125 to 0.03125
- queries: bfloat16 [256, 12288], P('dp'), may hold values from -0.0546875 to 0.0546875
Outputs:
- scores: float32 [256, 8], P('dp', 'fsdp')
The draws below stay inside these ranges and needn't reach their ends.
All inputs are finite; a program needn't handle non-finite values.
Results may differ from the reference program's by a relative error of at most 0.003.
Values may be sent and summed in bfloat16 or wider, within the bound.
A program may use at most 128 MiB of HBM per device.

```python
import jax
import jax.numpy as jnp
from jax import lax

D = 8192
FF = 28672
RANK = 64
SEQ_LEN = 128
QUERIES = 256
TOKENS = 1024


def steps_of(key, shape, split, least, high):
    level, own = 1.0, jax.random.fold_in(key, 6)
    for position, blocks in split:
        steps = jnp.exp(jax.random.uniform(jax.random.fold_in(own, position), (blocks,), jnp.float32, least / len(split), high / len(split)))
        level = level * jnp.repeat(steps, shape[position] // blocks).reshape([-1 if axis == position else 1 for axis in range(len(shape))])
    return level


def noise(rng, shape, width, bound, pieces=(), dtype=jnp.bfloat16):
    factor_of = steps_of(rng, shape, pieces, -0.22, 0.18) if pieces else 1.0
    result = jax.random.normal(rng, shape, jnp.float32) * width * factor_of
    return jnp.minimum(jnp.maximum(result, -bound), bound).astype(dtype)


def setup_inputs(seed: int = 0) -> dict:
    splits = jax.random.split(jax.random.key(seed), 9)
    tokens = noise(splits[0], (TOKENS, D), 1.0, 6.0, ((0, 4), (1, 16)))
    cotangent = noise(splits[1], (TOKENS, D), 1.0, 6.0, ((0, 4), (1, 16)))
    gate_weight = noise(splits[2], (D, FF), D ** -0.5, 0.0625, ((0, 4), (1, 64)))
    up_weight = noise(splits[3], (D, FF), D ** -0.5, 0.0625, ((0, 4), (1, 64)))
    down_weight = noise(splits[4], (FF, D), FF ** -0.5, 0.03125, ((0, 64), (1, 4)))
    model_projection = noise(splits[5], (RANK, D), D ** -0.5, 0.0625)
    hidden_projection = noise(splits[6], (RANK, FF), FF ** -0.5, 0.03125, ((1, 64),))
    queries = noise(splits[7], (QUERIES, 3 * RANK * RANK), (3 * RANK * RANK) ** -0.5, 0.0546875, ((0, 16),))
    return dict(tokens=tokens, cotangent=cotangent, gate_weight=gate_weight, up_weight=up_weight, down_weight=down_weight, model_projection=model_projection, hidden_projection=hidden_projection, queries=queries)


def reference(tokens, cotangent, gate_weight, up_weight, down_weight, model_projection, hidden_projection, queries):
    gate_pre = jnp.dot(tokens, gate_weight, preferred_element_type=jnp.float32)
    up_pre = jnp.dot(tokens, up_weight, preferred_element_type=jnp.float32)
    sigmoid_gate = jax.nn.sigmoid(gate_pre)
    activated = gate_pre * sigmoid_gate
    hidden = (activated * up_pre).astype(jnp.bfloat16)
    back_grad = jnp.dot(cotangent, down_weight.T, preferred_element_type=jnp.float32)
    grad_gate = (back_grad * up_pre * sigmoid_gate * (1.0 + gate_pre * (1.0 - sigmoid_gate))).astype(jnp.bfloat16)
    grad_up = (back_grad * activated).astype(jnp.bfloat16)
    model_tok = jnp.dot(tokens, model_projection.T, preferred_element_type=jnp.float32)
    model_cot = jnp.dot(cotangent, model_projection.T, preferred_element_type=jnp.float32)
    proj_gate = jnp.dot(grad_gate, hidden_projection.T, preferred_element_type=jnp.float32)
    proj_up = jnp.dot(grad_up, hidden_projection.T, preferred_element_type=jnp.float32)
    proj_hidden = jnp.dot(hidden, hidden_projection.T, preferred_element_type=jnp.float32)
    seq_count = tokens.shape[0] // SEQ_LEN

    def shaped(matrix):
        return matrix.reshape(seq_count, SEQ_LEN, RANK)

    high = lax.Precision.HIGHEST
    g_gate = jnp.einsum("sti,stj->sij", shaped(model_tok), shaped(proj_gate), precision=high)
    g_up = jnp.einsum("sti,stj->sij", shaped(model_tok), shaped(proj_up), precision=high)
    g_down = jnp.einsum("sti,stj->sij", shaped(proj_hidden), shaped(model_cot), precision=high)
    grads = jnp.stack((g_gate, g_up, g_down), axis=1).reshape(seq_count, 3 * RANK * RANK)
    return jnp.dot(queries.astype(jnp.float32), grads.T, precision=high)
```

```python
import jax
import jax.numpy as jnp
from jax import lax
from jax.experimental import pallas as pl
from jax.experimental.pallas import tpu as pltpu
from jax.sharding import PartitionSpec as P

MESH = pl.DeviceIdType.MESH
F32, BF16 = jnp.float32, jnp.bfloat16
SEQ_LEN = 128
NX, NY, NZ = 4, 4, 8
UP, DOWN = 2.0**40, 2.0**-20


def dot(a, b):
    return lax.dot_general(a, b, (((1,), (0,)), ((), ())), preferred_element_type=F32)


def dot_t(a, b):
    return lax.dot_general(a, b, (((1,), (1,)), ((), ())), preferred_element_type=F32)


def exact_dot(a, b):
    return lax.dot_general(
        a, b, (((1,), (0,)), ((), ())), precision=lax.Precision.HIGHEST, preferred_element_type=F32
    )


def encoded(v):
    return ((v * UP) * jnp.abs(v) * ((v * UP) * v)).astype(BF16)


def decoded(c):
    c = c.astype(F32)
    root = lax.rsqrt(lax.rsqrt(jnp.maximum(jnp.abs(c), 1e-37))) * DOWN
    return jnp.where(c < 0, -root, root)


def layer(gate, up, back):
    sig = jax.nn.sigmoid(gate)
    act = gate * sig
    hidden = (act * up).astype(BF16)
    grad_gate = (back * up * sig * (1.0 + gate * (1.0 - sig))).astype(BF16)
    grad_up = (back * act).astype(BF16)
    return grad_gate, grad_up, hidden


def kernel(
    tok, cot, wg, wu, wd, mp, hp, qs, out,
    loc, full, wg_v, wu_v, w_gu, wd_v, lb, lm, hpz, qv,
    enc, rh, rx, acc, ml, g_tmp, gpart, r8, s24, rz, gs,
    ld_sem, a_sem, b1_sem, b2_sem, c_sem, e_sem, d_sem, snd_sem, xs_sem, rh_sem, rx_sem, ml_sem, r8_sem, rz_sem, gs_sem,
):
    x = lax.axis_index("fsdp")
    t = lax.axis_index("tensor")
    d = lax.axis_index("dp")
    k, ylo = lax.rem(t, 2), t // 2
    yhi, z = d // NZ, lax.rem(d, NZ)
    y = yhi * 2 + ylo
    sib = 1 - k

    def dev(x_, y_, z_, k_):
        return (x_, lax.rem(y_, 2) * 2 + k_, (y_ // 2) * NZ + z_)

    def off(v, o, n):
        return lax.rem(v + o, n)

    def remote(src, dst, ssem, rsem, to):
        return pltpu.make_async_remote_copy(
            src_ref=src, dst_ref=dst, send_sem=ssem, recv_sem=rsem, device_id=to, device_id_type=MESH
        )

    def local(src, dst, sem):
        return pltpu.make_async_copy(src, dst, sem)

    def wait(ref, sem):
        pltpu.make_async_copy(ref, ref, sem).wait()

    @pl.when(k == 0)
    def _():
        local(tok, loc, ld_sem.at[0]).start()

    @pl.when(k == 1)
    def _():
        local(cot, loc, ld_sem.at[0]).start()

    depth = w_gu.shape[0]
    loads = [
        local(wg, wg_v, ld_sem.at[1]),
        local(wu, wu_v, ld_sem.at[2]),
        local(wd.at[pl.ds(0, 384)], wd_v, ld_sem.at[3]),
        local(wd.at[pl.ds(384, 64)], lb.at[pl.ds(0, 64)], ld_sem.at[4]),
        local(mp.at[:, pl.ds(pl.multiple_of(x * depth, depth), depth)], lm.at[pl.ds(64, 64)], ld_sem.at[5]),
        local(hp, hpz.at[pl.ds(64, 64)], ld_sem.at[6]),
        local(qs, qv, ld_sem.at[7]),
    ]
    for c in loads:
        c.start()

    barrier = pltpu.get_barrier_semaphore()
    peers = [
        dev(off(x, ox, NX), off(y, oy, NY), z, k) for ox in range(NX) for oy in range(NY) if ox or oy
    ]
    peers += [dev(x, y, off(z, oz, NZ), k) for oz in range(1, NZ)]
    peers += [dev(x, off(y, oy, NY), z, sib) for oy in range(NY)]
    for p in peers:
        pl.semaphore_signal(barrier, inc=1, device_id=p, device_id_type=MESH)
    pl.semaphore_wait(barrier, len(peers))

    def rows(r, q, part=0, n=64):
        return pl.ds(pl.multiple_of(r * 256 + q * 64 + part, 32), n)

    local(tok, loc, ld_sem.at[0]).wait()
    xt = 2 * yhi + z // 4
    y2 = off(y, 2 * ylo + 3, NY)
    col = pl.ds(pl.multiple_of(lax.rem(z, 4) * 512, 512), 512)

    def quarter(q):
        return loc.at[pl.ds(pl.multiple_of(q * 64, 64), 64)]

    a2 = remote(quarter(y2), full.at[k, rows(x, y2), col], snd_sem.at[0], a_sem.at[x], dev(xt, y2, z, k))
    a2.start()
    a1 = remote(quarter(y), full.at[k, rows(x, y), col], snd_sem.at[1], a_sem.at[x], dev(xt, y, z, k))

    @pl.when(xt != x)
    def _():
        a1.start()

    @pl.when(xt == x)
    def _():
        local(quarter(y), full.at[k, rows(x, y), col], a_sem.at[x]).start()

    for c in loads:
        c.wait()
    w_gu[:, 0:384] = wg_v[:, 0:384]
    w_gu[:, 384:768] = wu_v[:, 0:384]
    ri = lax.broadcasted_iota(jnp.int32, (64, 128), 0)
    ci = lax.broadcasted_iota(jnp.int32, (64, 128), 1)
    first = jnp.where(ri == ci, 1.0, 0.0).astype(BF16)
    second = jnp.where(ri + 64 == ci, 1.0, 0.0).astype(BF16)
    w_gu[:, 768:896] = (dot(wg_v[:, 384:448], first) + dot(wu_v[:, 384:448], second)).astype(BF16)
    lb[64:128, :] = jnp.zeros((64, depth), BF16)
    lm[0:64, :] = jnp.zeros((64, depth), BF16)
    hpz[0:64, :] = jnp.zeros((64, 448), BF16)
    hpz[128:192, :] = jnp.zeros((64, 448), BF16)

    order = (2, 1, 3, 0)
    rs = [off(x, o, NX) for o in order]
    zb = 4 * lax.rem(x, 2)
    is_src = z // 4 == lax.rem(x, 2)
    is_far = z // 4 != lax.rem(x, 2)
    far = lax.rem(z - zb + NZ, NZ)
    j = lax.rem(z, 4)

    @pl.when(is_src)
    def _():
        for r in rs:
            piece = full.at[k, rows(r, y), col]
            wait(piece, a_sem.at[r])
            targets = [zb + lax.rem(j + o, 4) for o in (1, 2, 3)]
            targets += [lax.rem(zb + 6 - 2 * (j // 2) + o, NZ) for o in (0, 1)]
            for zt in targets:
                remote(piece, piece, snd_sem.at[2], b1_sem.at[r], dev(x, y, zt, k)).start()

    def z_stage(i):
        r = rs[i]

        @pl.when(is_src)
        def _():
            wait(full.at[k, rows(r, y), pl.ds(0, 1536)], b1_sem.at[r])

        @pl.when(is_far)
        def _():
            wait(full.at[k, rows(r, y), pl.ds(0, 1024)], b1_sem.at[r])

            @pl.when(far == 5)
            def _():
                ref = full.at[k, rows(r, y), pl.ds(1024, 1024)]
                for o in (6, 7):
                    remote(ref, ref, snd_sem.at[3], b2_sem.at[r], dev(x, y, lax.rem(zb + o, NZ), k)).start()

            @pl.when(far == 6)
            def _():
                ref = full.at[k, rows(r, y), pl.ds(0, 1024)]
                for o in (5, 4):
                    remote(ref, ref, snd_sem.at[3], b2_sem.at[r], dev(x, y, lax.rem(zb + o, NZ), k)).start()

            wait(full.at[k, rows(r, y), pl.ds(0, 1024)], b2_sem.at[r])

    yp, ym, yo = off(y, 1, NY), off(y, 3, NY), off(y, 2, NY)

    def to_sibling(r, q):
        ref = full.at[k, rows(r, q)]
        remote(ref, ref, snd_sem.at[6], d_sem.at[r], dev(x, y, z, sib)).start()

    def y_send(i):
        r = rs[i]
        ref = full.at[k, rows(r, y)]
        remote(ref, ref, snd_sem.at[4], c_sem.at[0, r], dev(x, yp, z, k)).start()
        remote(ref, ref, snd_sem.at[4], c_sem.at[1, r], dev(x, ym, z, k)).start()
        to_sibling(r, y)

    def y_pass(i):
        r = rs[i]
        wait(full.at[k, rows(r, ym)], c_sem.at[0, r])
        ref = full.at[k, rows(r, ym, 0, 32)]
        remote(ref, ref, snd_sem.at[5], e_sem.at[0, r], dev(x, yp, z, k)).start()
        to_sibling(r, ym)
        wait(full.at[k, rows(r, yp)], c_sem.at[1, r])
        ref = full.at[k, rows(r, yp, 32, 32)]
        remote(ref, ref, snd_sem.at[5], e_sem.at[1, r], dev(x, ym, z, k)).start()
        to_sibling(r, yp)

    def y_done(i):
        r = rs[i]
        wait(full.at[k, rows(r, yo, 0, 32)], e_sem.at[0, r])
        wait(full.at[k, rows(r, yo, 32, 32)], e_sem.at[1, r])
        to_sibling(r, yo)
        wait(full.at[sib, pl.ds(pl.multiple_of(r * 256, 256), 256)], d_sem.at[r])

    def multiply(i, slot):
        block = pl.ds(pl.multiple_of(rs[i] * 256, 256), 256)
        acc[slot, :, 0:896] = dot(full[0, block, :], w_gu[...])
        acc[slot, :, 896:1280] = dot_t(full[1, block, :], wd_v[...])
        acc[slot, :, 1280:1408] = dot_t(full[1, block, :], lb[...]) + dot_t(full[k, block, :], lm[...])

    xp, xm = off(x, 1, NX), off(x, 3, NX)
    sends = []

    def x_send(src, dst, rsem, to):
        c = remote(src, dst, xs_sem.at[len(sends)], rsem, dev(to, y, z, k))
        c.start()
        sends.append(c)

    top, low = pl.ds(0, 128), pl.ds(128, 128)

    z_stage(0)
    y_send(0)
    z_stage(1)
    y_send(1)
    y_pass(0)
    y_done(0)
    multiply(0, 0)
    enc[0, 0:128] = encoded(acc[0, 0:128])
    x_send(enc.at[0, top], rh.at[0], rh_sem.at[0], xp)
    enc[0, 128:256] = encoded(acc[0, 128:256])
    x_send(enc.at[0, low], rh.at[1], rh_sem.at[1], xm)
    z_stage(2)
    y_send(2)
    y_pass(1)
    y_done(1)
    multiply(1, 0)
    enc[1, 128:256] = encoded(acc[0, 128:256])
    x_send(enc.at[1, low], rx.at[0, low], rx_sem.at[0, 1], xp)
    z_stage(3)
    y_send(3)
    y_pass(2)
    y_done(2)
    wait(rh.at[0], rh_sem.at[0])
    enc[1, 0:128] = encoded(acc[0, 0:128] + decoded(rh[0]))
    x_send(enc.at[1, top], rx.at[0, top], rx_sem.at[0, 0], xp)
    multiply(2, 1)
    enc[2, 0:128] = encoded(acc[1, 0:128])
    x_send(enc.at[2, top], rx.at[1, top], rx_sem.at[1, 0], xm)
    wait(rh.at[1], rh_sem.at[1])
    enc[2, 128:256] = encoded(acc[1, 128:256] + decoded(rh[1]))
    x_send(enc.at[2, low], rx.at[1, low], rx_sem.at[1, 1], xm)
    y_pass(3)
    y_done(3)
    multiply(3, 0)

    for s in range(2):
        part = pl.ds(s * 128, 128)
        wait(rx.at[0, part], rx_sem.at[0, s])
        wait(rx.at[1, part], rx_sem.at[1, s])
        acc[0, part] = acc[0, part] + decoded(rx[0, part]) + decoded(rx[1, part])
    ml[0] = acc[0, :, 1280:1408]
    model = remote(ml.at[0], ml.at[1], ml_sem.at[0], ml_sem.at[1], dev(x, y, z, sib))
    model.start()

    lane = lax.broadcasted_iota(jnp.int32, (32, 128), 1) < 64
    projected = []
    for s in range(2):
        part = pl.ds(s * 128, 128)
        gg, gu, hid = layer(acc[0, part, 0:384], acc[0, part, 384:768], acc[0, part, 896:1280])
        left = acc[0, part, 768:896]
        ggl, gul, hil = layer(left, pltpu.roll(left, 64, 1), acc[0, part, 1280:1408])
        pgu = dot_t(gg, hpz[64:192, 0:384]) + dot_t(ggl[:, 0:64], hpz[64:192, 384:448])
        pgu += dot_t(gu, hpz[0:128, 0:384]) + dot_t(gul[:, 0:64], hpz[0:128, 384:448])
        ph = dot_t(hid, hpz[64:192, 0:384]) + dot_t(hil[:, 0:64], hpz[64:192, 384:448])
        projected.append((pgu, ph))
    model.wait()
    for s in range(2):
        part = pl.ds(s * 128, 128)
        pgu, ph = projected[s]
        mine, other = ml[0, part], ml[1, part]
        m_tok = jnp.where(k == 0, mine, other)
        m_cot = jnp.where(k == 0, other, mine)
        g_tmp[0] = exact_dot(m_tok.T, pgu)
        g_tmp[1] = exact_dot(ph.T, m_cot)
        even, odd = g_tmp[0, pl.ds(64, 32, 2), :], g_tmp[0, pl.ds(65, 32, 2), :]
        gpart[s, 0:32] = jnp.where(lane, even, pltpu.roll(odd, 64, 1))
        gpart[s, 32:64] = jnp.where(lane, pltpu.roll(even, 64, 1), odd)
        even, odd = g_tmp[1, pl.ds(0, 32, 2), :], g_tmp[1, pl.ds(1, 32, 2), :]
        gpart[s, 64:96] = jnp.where(lane, pltpu.roll(even, 64, 1), odd)

    def share(q):
        return pl.ds(pl.multiple_of(q * 24, 8), 24)

    near = [(oy, ok) for oy in range(NY) for ok in range(2) if oy or ok]
    for n, (oy, ok) in enumerate(near):
        y_, k_ = off(y, oy, NY), off(k, ok, 2)
        remote(gpart.at[k_, share(y_)], r8.at[n], snd_sem.at[7], r8_sem.at[n], dev(x, y_, z, k_)).start()
    total = gpart[k, share(y)]
    for n in range(7):
        wait(r8.at[n], r8_sem.at[n])
        total += r8[n]
    s24[...] = total
    for n in range(7):
        remote(s24, rz.at[n], snd_sem.at[8], rz_sem.at[n], dev(x, y, off(z, n + 1, NZ), k)).start()
    for n in range(7):
        wait(rz.at[n], rz_sem.at[n])
        total += rz[n]
    gs[k, share(y)] = total
    for n, (oy, ok) in enumerate(near):
        y_, k_ = off(y, oy, NY), off(k, ok, 2)
        ref = gs.at[k, share(y)]
        remote(ref, ref, snd_sem.at[9], gs_sem.at[n], dev(x, y_, z, k_)).start()
    for n in range(7):
        wait(r8.at[n], gs_sem.at[n])

    sums = [jnp.zeros((16, 128), F32), jnp.zeros((16, 128), F32)]
    for p in range(96):
        q = qv[:, p * 128 : (p + 1) * 128].astype(F32)
        for s in range(2):
            sums[s] += q * gs[s, p : p + 1, :]
    two = lax.broadcasted_iota(jnp.int32, (16, 2), 1)
    out[...] = jnp.where(two == 0, sums[0].sum(1, keepdims=True), sums[1].sum(1, keepdims=True))

    a2.wait_send()

    @pl.when(xt != x)
    def _():
        a1.wait_send()

    @pl.when(is_src)
    def _():
        wait(full.at[0, pl.ds(0, 320)], snd_sem.at[2])

    @pl.when((far == 5) | (far == 6))
    def _():
        wait(full.at[0, pl.ds(0, 256)], snd_sem.at[3])

    wait(full.at[0, pl.ds(0, 512)], snd_sem.at[4])
    wait(full.at[0, pl.ds(0, 256)], snd_sem.at[5])
    wait(full.at[0], snd_sem.at[6])
    for c in sends:
        c.wait_send()
    for n in (7, 8, 9):
        wait(r8, snd_sem.at[n])


def on_device(tok, cot, wg, wu, wd, mp, hp, qs):
    depth = wg.shape[0]
    any_ = pl.BlockSpec(memory_space=pl.ANY)
    dma = pltpu.SemaphoreType.DMA
    return pl.pallas_call(
        kernel,
        out_shape=jax.ShapeDtypeStruct((16, 2), F32),
        in_specs=[any_] * 8,
        out_specs=pl.BlockSpec(memory_space=pltpu.VMEM),
        scratch_shapes=[
            pltpu.VMEM((256, 512), BF16),
            pltpu.VMEM((2, 1024, depth), BF16),
            pltpu.VMEM((depth, 448), BF16),
            pltpu.VMEM((depth, 448), BF16),
            pltpu.VMEM((depth, 896), BF16),
            pltpu.VMEM((384, depth), BF16),
            pltpu.VMEM((128, depth), BF16),
            pltpu.VMEM((128, depth), BF16),
            pltpu.VMEM((192, 448), BF16),
            pltpu.VMEM((16, 12288), BF16),
            pltpu.VMEM((3, 256, 1408), BF16),
            pltpu.VMEM((2, 128, 1408), BF16),
            pltpu.VMEM((2, 256, 1408), BF16),
            pltpu.VMEM((2, 256, 1408), F32),
            pltpu.VMEM((2, 256, 128), F32),
            pltpu.VMEM((2, 128, 128), F32),
            pltpu.VMEM((2, 96, 128), F32),
            pltpu.VMEM((7, 24, 128), F32),
            pltpu.VMEM((24, 128), F32),
            pltpu.VMEM((7, 24, 128), F32),
            pltpu.VMEM((2, 96, 128), F32),
            dma((8,)),
            dma((4,)),
            dma((4,)),
            dma((4,)),
            dma((2, 4)),
            dma((2, 4)),
            dma((4,)),
            dma((10,)),
            dma((6,)),
            dma((2,)),
            dma((2, 2)),
            dma((2,)),
            dma((7,)),
            dma((7,)),
            dma((7,)),
        ],
        compiler_params=pltpu.CompilerParams(
            collective_id=0, has_side_effects=True, vmem_limit_bytes=60 * 2**20
        ),
        name="grads_and_scores",
    )(tok, cot, wg, wu, wd, mp, hp, qs)


def solution(mesh):
    return jax.shard_map(
        on_device,
        mesh=mesh,
        in_specs=(
            P("fsdp", "dp"),
            P("fsdp", "dp"),
            P("fsdp", ("tensor", "dp")),
            P("fsdp", ("tensor", "dp")),
            P(("tensor", "dp"), "fsdp"),
            P(),
            P(None, ("tensor", "dp")),
            P("dp", None),
        ),
        out_specs=P("dp", "fsdp"),
        check_vma=False,
    )
```

```python
import functools

import jax
import jax.numpy as jnp
from jax import lax
from jax.experimental import pallas as pl
from jax.experimental.pallas import tpu as pltpu
from jax.sharding import PartitionSpec as P

MESH = pl.DeviceIdType.MESH
F32, BF16 = jnp.float32, jnp.bfloat16
SEQ_LEN = 128
NX, NY, NZ = 4, 4, 8
UP, DOWN = 2.0**40, 2.0**-20


def dot(a, b):
    return lax.dot_general(a, b, (((1,), (0,)), ((), ())), preferred_element_type=F32)


def dot_t(a, b):
    return lax.dot_general(a, b, (((1,), (1,)), ((), ())), preferred_element_type=F32)


def exact_dot(a, b):
    return lax.dot_general(
        a, b, (((1,), (0,)), ((), ())), precision=lax.Precision.HIGHEST, preferred_element_type=F32
    )


def encoded(v):
    return ((v * UP) * jnp.abs(v) * ((v * UP) * v)).astype(BF16)


def decoded(c):
    c = c.astype(F32)
    root = lax.rsqrt(lax.rsqrt(jnp.maximum(jnp.abs(c), 1e-37))) * DOWN
    return jnp.where(c < 0, -root, root)


def layer(gate, up, back):
    sig = jax.nn.sigmoid(gate)
    act = gate * sig
    hidden = (act * up).astype(BF16)
    grad_gate = (back * up * sig * (1.0 + gate * (1.0 - sig))).astype(BF16)
    grad_up = (back * act).astype(BF16)
    return grad_gate, grad_up, hidden


def kernel(
    tok, cot, wg, wu, wd, mp, hp, qs, out,
    loc, full, w_gu, w_b, hpz, qv,
    enc, rh, rx, acc, ml, g_tmp, gpart, r8, s24, rz, gs,
    ld_sem, a_sem, z_sem, y_sem, d_sem, snd_sem, a_snd, xs_sem, rh_sem, rx_sem, ml_sem, r8_sem, rz_sem, gs_sem,
):
    x = lax.axis_index("fsdp")
    t = lax.axis_index("tensor")
    d = lax.axis_index("dp")
    k, ylo = lax.rem(t, 2), t // 2
    yhi, z = d // NZ, lax.rem(d, NZ)
    y = yhi * 2 + ylo
    sib = 1 - k

    def dev(x_, y_, z_, k_):
        return (x_, lax.rem(y_, 2) * 2 + k_, (y_ // 2) * NZ + z_)

    def off(v, o, n):
        return lax.rem(v + o, n)

    def remote(src, dst, ssem, rsem, to):
        return pltpu.make_async_remote_copy(
            src_ref=src, dst_ref=dst, send_sem=ssem, recv_sem=rsem, device_id=to, device_id_type=MESH
        )

    def local(src, dst, sem):
        return pltpu.make_async_copy(src, dst, sem)

    def wait(ref, sem):
        pltpu.make_async_copy(ref, ref, sem).wait()

    @pl.when(k == 0)
    def _():
        local(tok, loc, ld_sem.at[0]).start()

    @pl.when(k == 1)
    def _():
        local(cot, loc, ld_sem.at[0]).start()

    depth = w_gu.shape[1]
    mp_own = mp.at[:, pl.ds(pl.multiple_of(x * depth, depth), depth)]
    loads = [
        local(wg.at[pl.ds(0, 384)], w_gu.at[pl.ds(0, 384)], ld_sem.at[1]),
        local(wu.at[pl.ds(0, 384)], w_gu.at[pl.ds(384, 384)], ld_sem.at[2]),
        local(wg.at[pl.ds(384, 64)], w_gu.at[pl.ds(768, 64)], ld_sem.at[3]),
        local(wu.at[pl.ds(384, 64)], w_gu.at[pl.ds(832, 64)], ld_sem.at[4]),
        local(mp_own, w_gu.at[pl.ds(960, 64)], ld_sem.at[5]),
        local(wd, w_b.at[pl.ds(0, 448)], ld_sem.at[6]),
        local(mp_own, w_b.at[pl.ds(448, 64)], ld_sem.at[7]),
        local(hp, hpz.at[pl.ds(64, 64)], ld_sem.at[8]),
        local(qs, qv, ld_sem.at[9]),
    ]
    for c in loads:
        c.start()

    barrier = pltpu.get_barrier_semaphore()
    peers = [
        dev(off(x, ox, NX), off(y, oy, NY), z, k) for ox in range(NX) for oy in range(NY) if ox or oy
    ]
    peers += [dev(x, y, off(z, oz, NZ), k) for oz in range(1, NZ)]
    peers += [dev(x, off(y, oy, NY), z, sib) for oy in range(NY)]
    peers += [
        dev(off(x, ox, NX), off(y, oy, NY), off(z, oz, NZ), k)
        for ox in range(NX) for oy in (0, 1, 3) for oz in (1, 2, 6, 7) if ox or oy
    ]
    for p in peers:
        pl.semaphore_signal(barrier, inc=1, device_id=p, device_id_type=MESH)
    pl.semaphore_wait(barrier, len(peers))

    def rows(r, p, part=0, n=128):
        return pl.ds(pl.multiple_of(r * 256 + p * 128 + part, 32), n)

    def piece(r, p, v, part=0, n=64):
        return full.at[k, rows(r, p, lax.rem(v, 2) * 64 + part, n), pl.ds(pl.multiple_of(v // 2 * 512, 512), 512)]

    local(tok, loc, ld_sem.at[0]).wait()
    xt = 2 * yhi + z // 4
    y2 = off(y, 2 * ylo + 3, NY)
    j = lax.rem(z, 4)
    me_p = lax.rem(y, 2)
    a_sends = []
    for n, (yt, u) in enumerate(((y2, 0), (y2, 1), (y, 0), (y, 1))):
        p = lax.rem(yt, 2)
        src = loc.at[pl.ds(pl.multiple_of(p * 128 + u * 64, 64), 64)]
        dst = piece(x, p, 2 * j + u)
        zt = lax.rem(z + j + u + NZ - 2, NZ)
        c = remote(src, dst, a_snd.at[n], a_sem.at[x], dev(xt, yt, zt, k))
        here = (xt == x) & (j + u == 2) if n >= 2 else None
        a_sends.append((c, here))
        if here is None:
            c.start()
        else:

            @pl.when(jnp.logical_not(here))
            def _(c=c):
                c.start()

            @pl.when(here)
            def _(src=src, dst=dst):
                local(src, dst, a_sem.at[x]).start()

    w_gu[896:960, :] = jnp.zeros((64, depth), BF16)
    hpz[0:64, :] = jnp.zeros((64, 448), BF16)
    hpz[128:192, :] = jnp.zeros((64, 448), BF16)

    order = (2, 1, 3, 0)
    rs = [off(x, o, NX) for o in order]
    zb = 4 * lax.rem(x, 2)
    w = lax.rem(z - zb + 2 + NZ, NZ)
    zp, zm = off(z, 1, NZ), off(z, NZ - 1, NZ)
    yp, ym = off(y, 1, NY), off(y, 3, NY)

    def place(o):
        return lax.rem(w + o + NZ, NZ)

    def along_z(ref, up, r, s):
        remote(ref, ref, snd_sem.at[0], z_sem.at[1 - up, r, s], dev(x, y, zp if up else zm, k)).start()

    def along_y(r, v):
        ref = piece(r, me_p, v)
        to = jnp.where(lax.rem(v, 2) == 0, yp, ym)
        remote(ref, ref, snd_sem.at[1], y_sem.at[r], dev(x, to, z, k)).start()

    def z_step(i, s):
        r = rs[i]
        if s == 0:
            own = piece(r, me_p, w)
            wait(own, a_sem.at[r])
            along_z(own, 1, r, 0)
            along_z(own, 0, r, 0)
            along_y(r, w)
        elif s < 4:
            for up in (1, 0):
                v = place(-s if up else s)
                got = piece(r, me_p, v)
                wait(got, z_sem.at[1 - up, r, s - 1])
                if s < 3:
                    along_z(got, up, r, s)
                else:
                    along_z(piece(r, me_p, v, 0 if up else 32, 32), up, r, s)
                along_y(r, v)
        else:
            v = place(4)
            wait(piece(r, me_p, v, 0, 32), z_sem.at[0, r, 3])
            wait(piece(r, me_p, v, 32, 32), z_sem.at[1, r, 3])
            along_y(r, v)
            ref = full.at[k, rows(r, me_p)]
            remote(ref, ref, snd_sem.at[2], d_sem.at[r], dev(x, y, z, sib)).start()

    def y_step(i):
        r = rs[i]
        ref = full.at[k, rows(r, 1 - me_p)]
        wait(ref, y_sem.at[r])
        remote(ref, ref, snd_sem.at[2], d_sem.at[r], dev(x, y, z, sib)).start()

    slots = (0, 1, 2, 0)

    def block(i):
        return pl.ds(pl.multiple_of(rs[i] * 256, 256), 256)

    def multiply_gu(i):
        wait(full.at[sib, block(i)], d_sem.at[rs[i]])
        acc[slots[i], :, 0:1024] = dot_t(full[0, block(i), :], w_gu[...])

    left_lanes = lax.broadcasted_iota(jnp.int32, (256, 128), 1) < 64

    def multiply_b(i):
        slot = slots[i]
        acc[slot, :, 1024:1536] = dot_t(full[1, block(i), :], w_b[...])
        both = acc[slot, :, 1408:1536]
        acc[slot, :, 896:1024] = jnp.where(left_lanes | (k == 1), both, acc[slot, :, 896:1024])

    xp, xm = off(x, 1, NX), off(x, 3, NX)
    sends = []

    def x_send(src, dst, rsem, to):
        c = remote(src, dst, xs_sem.at[len(sends)], rsem, dev(to, y, z, k))
        c.start()
        sends.append(c)

    def x_put(i, h, dst, rsem, to, plus=None):
        part = pl.ds(h * 128, 128)
        v = acc[slots[i], part, 0:1408]
        if plus is not None:
            v = v + decoded(plus)
        enc[i, part] = encoded(v)
        x_send(enc.at[i, part], dst, rsem, to)

    top, low = pl.ds(0, 128), pl.ds(128, 128)

    def x_step(i):
        if i == 0:
            x_put(0, 0, rh.at[0], rh_sem.at[0], xp)
            x_put(0, 1, rh.at[1], rh_sem.at[1], xm)
        elif i == 1:
            x_put(1, 1, rx.at[0, low], rx_sem.at[0, 1], xp)
        elif i == 2:
            x_put(2, 0, rx.at[1, top], rx_sem.at[1, 0], xm)

    def x_last(h):
        wait(rh.at[h], rh_sem.at[h])
        if h == 0:
            x_put(1, 0, rx.at[0, top], rx_sem.at[0, 0], xp, rh[0])
        else:
            x_put(2, 1, rx.at[1, low], rx_sem.at[1, 1], xm, rh[1])

    events = []
    starts = (0, 1, 3, 5)
    for i, at in enumerate(starts):
        for s in range(5):
            events.append((at + s, 0, i, "z%d_%d" % (i, s), functools.partial(z_step, i, s)))
        events.append((at + 5, 1, i, "y%d" % i, functools.partial(y_step, i)))
        events.append((at + 6, 2, i, "gu%d" % i, functools.partial(multiply_gu, i)))
        events.append((at + 7, 2, i, "b%d" % i, functools.partial(multiply_b, i)))
        events.append((at + 7, 3, i, "x%d" % i, functools.partial(x_step, i)))
    events.append((11, 4, 0, "xl0", functools.partial(x_last, 0)))
    events.append((12, 4, 1, "xl1", functools.partial(x_last, 1)))
    events.sort(key=lambda e: e[:3])
    waited = False
    for e in events:
        if e[3] == "gu0":
            for c in loads:
                c.wait()
        with jax.named_scope(e[3]):
            e[4]()

    for s in range(2):
        part = pl.ds(s * 128, 128)
        wait(rx.at[0, part], rx_sem.at[0, s])
        wait(rx.at[1, part], rx_sem.at[1, s])
        acc[0, part, 0:1408] = acc[0, part, 0:1408] + decoded(rx[0, part]) + decoded(rx[1, part])
    ml[0] = acc[0, :, 896:1024]
    model = remote(ml.at[0], ml.at[1], ml_sem.at[0], ml_sem.at[1], dev(x, y, z, sib))
    model.start()

    lane = lax.broadcasted_iota(jnp.int32, (32, 128), 1) < 64
    projected = []
    for s in range(2):
        part = pl.ds(s * 128, 128)
        gg, gu, hid = layer(acc[0, part, 0:384], acc[0, part, 384:768], acc[0, part, 1024:1408])
        left = acc[0, part, 768:896]
        ggl, gul, hil = layer(left, pltpu.roll(left, 64, 1), acc[0, part, 896:1024])
        pgu = dot_t(gg, hpz[64:192, 0:384]) + dot_t(ggl[:, 0:64], hpz[64:192, 384:448])
        pgu += dot_t(gu, hpz[0:128, 0:384]) + dot_t(gul[:, 0:64], hpz[0:128, 384:448])
        ph = dot_t(hid, hpz[64:192, 0:384]) + dot_t(hil[:, 0:64], hpz[64:192, 384:448])
        projected.append((pgu, ph))
    model.wait()
    for s in range(2):
        part = pl.ds(s * 128, 128)
        pgu, ph = projected[s]
        mine, other = ml[0, part], ml[1, part]
        m_tok = jnp.where(k == 0, mine, other)
        m_cot = jnp.where(k == 0, other, mine)
        g_tmp[0] = exact_dot(m_tok.T, pgu)
        g_tmp[1] = exact_dot(ph.T, m_cot)
        even, odd = g_tmp[0, pl.ds(64, 32, 2), :], g_tmp[0, pl.ds(65, 32, 2), :]
        gpart[s, 0:32] = jnp.where(lane, even, pltpu.roll(odd, 64, 1))
        gpart[s, 32:64] = jnp.where(lane, pltpu.roll(even, 64, 1), odd)
        even, odd = g_tmp[1, pl.ds(0, 32, 2), :], g_tmp[1, pl.ds(1, 32, 2), :]
        gpart[s, 64:96] = jnp.where(lane, pltpu.roll(even, 64, 1), odd)

    def share(q):
        return pl.ds(pl.multiple_of(q * 24, 8), 24)

    near = [(oy, ok) for oy in range(NY) for ok in range(2) if oy or ok]
    for n, (oy, ok) in enumerate(near):
        y_, k_ = off(y, oy, NY), off(k, ok, 2)
        remote(gpart.at[k_, share(y_)], r8.at[n], snd_sem.at[7], r8_sem.at[n], dev(x, y_, z, k_)).start()
    total = gpart[k, share(y)]
    for n in range(7):
        wait(r8.at[n], r8_sem.at[n])
        total += r8[n]
    s24[...] = total
    for n in range(7):
        remote(s24, rz.at[n], snd_sem.at[8], rz_sem.at[n], dev(x, y, off(z, n + 1, NZ), k)).start()
    for n in range(7):
        wait(rz.at[n], rz_sem.at[n])
        total += rz[n]
    gs[k, share(y)] = total
    for n, (oy, ok) in enumerate(near):
        y_, k_ = off(y, oy, NY), off(k, ok, 2)
        ref = gs.at[k, share(y)]
        remote(ref, ref, snd_sem.at[9], gs_sem.at[n], dev(x, y_, z, k_)).start()
    for n in range(7):
        wait(r8.at[n], gs_sem.at[n])

    sums = [jnp.zeros((16, 128), F32), jnp.zeros((16, 128), F32)]
    for p in range(96):
        q = qv[:, p * 128 : (p + 1) * 128].astype(F32)
        for s in range(2):
            sums[s] += q * gs[s, p : p + 1, :]
    two = lax.broadcasted_iota(jnp.int32, (16, 2), 1)
    out[...] = jnp.where(two == 0, sums[0].sum(1, keepdims=True), sums[1].sum(1, keepdims=True))

    for c, here in a_sends:
        if here is None:
            c.wait_send()
        else:

            @pl.when(jnp.logical_not(here))
            def _(c=c):
                c.wait_send()

    wait(full.at[0, pl.ds(0, 448)], snd_sem.at[0])
    wait(full.at[0, pl.ds(0, 512)], snd_sem.at[1])
    wait(full.at[0], snd_sem.at[2])
    for c in sends:
        c.wait_send()
    for n in (7, 8, 9):
        wait(r8, snd_sem.at[n])


def on_device(tok, cot, wg, wu, wd, mp, hp, qs):
    depth = wg.shape[0]
    wg, wu = wg.T, wu.T
    any_ = pl.BlockSpec(memory_space=pl.ANY)
    dma = pltpu.SemaphoreType.DMA
    return pl.pallas_call(
        kernel,
        out_shape=jax.ShapeDtypeStruct((16, 2), F32),
        in_specs=[any_] * 8,
        out_specs=pl.BlockSpec(memory_space=pltpu.VMEM),
        scratch_shapes=[
            pltpu.VMEM((256, 512), BF16),
            pltpu.VMEM((2, 1024, depth), BF16),
            pltpu.VMEM((1024, depth), BF16),
            pltpu.VMEM((512, depth), BF16),
            pltpu.VMEM((192, 448), BF16),
            pltpu.VMEM((16, 12288), BF16),
            pltpu.VMEM((3, 256, 1408), BF16),
            pltpu.VMEM((2, 128, 1408), BF16),
            pltpu.VMEM((2, 256, 1408), BF16),
            pltpu.VMEM((3, 256, 1536), F32),
            pltpu.VMEM((2, 256, 128), F32),
            pltpu.VMEM((2, 128, 128), F32),
            pltpu.VMEM((2, 96, 128), F32),
            pltpu.VMEM((7, 24, 128), F32),
            pltpu.VMEM((24, 128), F32),
            pltpu.VMEM((7, 24, 128), F32),
            pltpu.VMEM((2, 96, 128), F32),
            dma((10,)),
            dma((4,)),
            dma((2, 4, 4)),
            dma((4,)),
            dma((4,)),
            dma((10,)),
            dma((4,)),
            dma((6,)),
            dma((2,)),
            dma((2, 2)),
            dma((2,)),
            dma((7,)),
            dma((7,)),
            dma((7,)),
        ],
        compiler_params=pltpu.CompilerParams(
            collective_id=0, has_side_effects=True, vmem_limit_bytes=60 * 2**20
        ),
        name="grads_and_scores",
    )(tok, cot, wg, wu, wd, mp, hp, qs)


def solution(mesh):
    return jax.shard_map(
        on_device,
        mesh=mesh,
        in_specs=(
            P("fsdp", "dp"),
            P("fsdp", "dp"),
            P("fsdp", ("tensor", "dp")),
            P("fsdp", ("tensor", "dp")),
            P(("tensor", "dp"), "fsdp"),
            P(),
            P(None, ("tensor", "dp")),
            P("dp", None),
        ),
        out_specs=P("dp", "fsdp"),
        check_vma=False,
    )
```

```python
import functools

import jax
import jax.numpy as jnp
from jax import lax
from jax.experimental import pallas as pl
from jax.experimental.pallas import tpu as pltpu
from jax.sharding import PartitionSpec as P

MESH = pl.DeviceIdType.MESH
F32, BF16 = jnp.float32, jnp.bfloat16
SEQ_LEN = 128
NX, NY, NZ = 4, 4, 8
SCHEDULE = (
    "z0_0", "a1", "z0_1", "z0_2", "z0_3", "z1_0", "z0_4", "z1_1", "y0n", "m0", "x0", "y0s", "z1_2", "z1_3", "m1",
    "x1", "z1_4", "y1n", "m2", "x2", "y1s", "m3",
)
PARTS = 1
UP, DOWN = 2.0**40, 2.0**-20


def dot(a, b):
    return lax.dot_general(a, b, (((1,), (0,)), ((), ())), preferred_element_type=F32)


def dot_t(a, b):
    return lax.dot_general(a, b, (((1,), (1,)), ((), ())), preferred_element_type=F32)


def exact_dot(a, b):
    return lax.dot_general(
        a, b, (((1,), (0,)), ((), ())), precision=lax.Precision.HIGHEST, preferred_element_type=F32
    )


def encoded(v):
    return ((v * UP) * jnp.abs(v) * ((v * UP) * v)).astype(BF16)


def decoded(c):
    c = c.astype(F32)
    root = lax.rsqrt(lax.rsqrt(jnp.maximum(jnp.abs(c), 1e-37))) * DOWN
    return jnp.where(c < 0, -root, root)


def layer(gate, up, back):
    sig = jax.nn.sigmoid(gate)
    act = gate * sig
    hidden = (act * up).astype(BF16)
    grad_gate = (back * up * sig * (1.0 + gate * (1.0 - sig))).astype(BF16)
    grad_up = (back * act).astype(BF16)
    return grad_gate, grad_up, hidden


def kernel(
    tok, cot, wg, wu, wd, mp, hp, qs, out,
    loc, full, w_gu, w_b, hpz, qv,
    enc, rh, rx, acc, ml, g_tmp, gpart, r8, s24, rz, gs,
    ld_sem, a_sem, z_sem, y_sem, d_sem, snd_sem, a_snd, xs_sem, rh_sem, rx_sem, ml_sem, r8_sem, rz_sem, gs_sem,
):
    x = lax.axis_index("fsdp")
    t = lax.axis_index("tensor")
    d = lax.axis_index("dp")
    k, ylo = lax.rem(t, 2), t // 2
    yhi, z = d // NZ, lax.rem(d, NZ)
    y = yhi * 2 + ylo
    sib = 1 - k

    def dev(x_, y_, z_, k_):
        return (x_, lax.rem(y_, 2) * 2 + k_, (y_ // 2) * NZ + z_)

    def off(v, o, n):
        return lax.rem(v + o, n)

    def remote(src, dst, ssem, rsem, to):
        return pltpu.make_async_remote_copy(
            src_ref=src, dst_ref=dst, send_sem=ssem, recv_sem=rsem, device_id=to, device_id_type=MESH
        )

    def local(src, dst, sem):
        return pltpu.make_async_copy(src, dst, sem)

    def wait(ref, sem):
        pltpu.make_async_copy(ref, ref, sem).wait()

    own_loads = [local(tok, loc.at[0], ld_sem.at[0]), local(cot, loc.at[1], ld_sem.at[10])]
    for c in own_loads:
        c.start()

    depth = w_gu.shape[1]
    mp_own = mp.at[:, pl.ds(pl.multiple_of(x * depth, depth), depth)]
    loads = [
        local(wg.at[pl.ds(0, 384)], w_gu.at[pl.ds(0, 384)], ld_sem.at[1]),
        local(wu.at[pl.ds(0, 384)], w_gu.at[pl.ds(384, 384)], ld_sem.at[2]),
        local(wg.at[pl.ds(384, 64)], w_gu.at[pl.ds(768, 64)], ld_sem.at[3]),
        local(wu.at[pl.ds(384, 64)], w_gu.at[pl.ds(832, 64)], ld_sem.at[4]),
        local(mp_own, w_gu.at[pl.ds(960, 64)], ld_sem.at[5]),
        local(wd, w_b.at[pl.ds(0, 448)], ld_sem.at[6]),
        local(mp_own, w_b.at[pl.ds(448, 64)], ld_sem.at[7]),
        local(hp, hpz.at[pl.ds(64, 64)], ld_sem.at[8]),
        local(qs, qv, ld_sem.at[9]),
    ]
    for c in loads:
        c.start()

    barrier = pltpu.get_barrier_semaphore()
    peers = [
        dev(off(x, ox, NX), off(y, oy, NY), z, k) for ox in range(NX) for oy in range(NY) if ox or oy
    ]
    peers += [dev(x, y, off(z, oz, NZ), k) for oz in range(1, NZ)]
    peers += [dev(x, off(y, oy, NY), z, sib) for oy in range(NY)]
    peers += [
        dev(off(x, ox, NX), off(y, oy, NY), off(z, oz, NZ), k)
        for ox in range(NX) for oy in (0, 1, 3) for oz in (1, 2, 6, 7) if ox or oy
    ]
    for p in peers:
        pl.semaphore_signal(barrier, inc=1, device_id=p, device_id_type=MESH)
    pl.semaphore_wait(barrier, len(peers))

    def rows(i, p, part=0, n=128):
        return pl.ds(pl.multiple_of(i * 256 + p * 128 + part, 32), n)

    def piece(a, i, p, v, part=0, n=64):
        at = rows(i, p, lax.rem(v, 2) * 64 + part, n)
        return full.at[a, at, pl.ds(pl.multiple_of(v // 2 * 512, 512), 512)]

    chunks = [(a, h, 64 // PARTS) for a in range(2) for h in range(0, 64, 64 // PARTS)]

    def mine(n):
        return 2 * n + 1 - k

    for c in own_loads:
        c.wait()
    xt = 2 * yhi + z // 4
    y2 = off(y, 2 * ylo + 3, NY)
    j = lax.rem(z, 4)
    me_p = lax.rem(y, 2)
    away = lax.rem(x - xt + NX, NX)
    a_sends = []
    for n, (yt, u) in enumerate(((y2, 0), (y2, 1), (y, 0), (y, 1))):
        p = lax.rem(yt, 2)
        slot = jnp.where(away == 2, 0, jnp.where(away == 0, 3, 2 - lax.rem(away // 2 + p, 2)))
        zt = lax.rem(z + j + u + NZ - 2, NZ)
        here = (xt == x) & (j + u == 2) if n >= 2 else xt != xt
        for m, (a, h, rows_) in enumerate(chunks):
            src = loc.at[a, pl.ds(pl.multiple_of(p * 128 + u * 64 + h, 32), rows_)]
            dst = piece(a, slot, p, 2 * j + u, h, rows_)
            c = remote(src, dst, a_snd.at[n, m], a_sem.at[slot, m], dev(xt, yt, zt, k))
            a_sends.append((m, c, here, slot, local(src, dst, a_sem.at[slot, m])))
    a_sends.sort(key=lambda e: e[0])

    def a_step(n):
        for _, c, here, slot, stay in a_sends:

            @pl.when((slot == mine(n)) & jnp.logical_not(here))
            def _(c=c):
                c.start()

            @pl.when((slot == mine(n)) & here)
            def _(stay=stay):
                stay.start()

    a_step(0)
    w_gu[896:960, :] = jnp.zeros((64, depth), BF16)
    hpz[0:64, :] = jnp.zeros((64, 448), BF16)
    hpz[128:192, :] = jnp.zeros((64, 448), BF16)

    zb = 4 * lax.rem(x, 2)
    w = lax.rem(z - zb + 2 + NZ, NZ)
    zp, zm = off(z, 1, NZ), off(z, NZ - 1, NZ)
    yp, ym = off(y, 1, NY), off(y, 3, NY)

    def place(o):
        return lax.rem(w + o + NZ, NZ)

    def along_z(ref, to, i, way, s, m):
        remote(ref, ref, snd_sem.at[0], z_sem.at[way, i, s, m], dev(x, y, to, k)).start()

    def along_y(a, i, v, h, n):
        ref = piece(a, i, me_p, v, h, n)
        to = jnp.where(lax.rem(v, 2) == 0, yp, ym)
        remote(ref, ref, snd_sem.at[1], y_sem.at[i, a], dev(x, to, z, k)).start()

    def to_sibling(a, i, p):
        ref = full.at[a, rows(i, p)]
        remote(ref, ref, snd_sem.at[2], d_sem.at[i, a], dev(x, y, z, sib)).start()

    def z_step(n, s):
        i = mine(n)
        for m, (a, h, rows_) in enumerate(chunks):
            if s == 0:
                own = piece(a, i, me_p, w, h, rows_)
                wait(own, a_sem.at[i, m])
                along_z(own, zp, i, 0, 0, m)
                along_z(own, zm, i, 1, 0, m)
                along_y(a, i, w, h, rows_)
            elif s < 4:
                for way in range(2):
                    v = place(s if way else -s)
                    got = piece(a, i, me_p, v, h, rows_)
                    wait(got, z_sem.at[way, i, s - 1, m])
                    to = zm if way else zp
                    if s < 3:
                        along_z(got, to, i, way, s, m)
                    elif PARTS == 1:
                        along_z(piece(a, i, me_p, v, 32 * way, 32), to, i, way, s, m)
                    elif h == 32 * way:
                        along_z(got, to, i, way, s, m)
                    along_y(a, i, v, h, rows_)
            else:
                v = place(4)
                for way in range(2):
                    if PARTS == 1 or h == 32 * way:
                        wait(piece(a, i, me_p, v, 32 * way, 32), z_sem.at[way, i, 3, m])
                along_y(a, i, v, h, rows_)
                if m % PARTS == PARTS - 1:
                    to_sibling(a, i, me_p)

    def y_step(n, who):
        @pl.when(k == who)
        def _():
            i = mine(n)
            for a in range(2):
                wait(full.at[a, rows(i, 1 - me_p)], y_sem.at[i, a])
                to_sibling(a, i, 1 - me_p)

    slots = (0, 1, 2, 0)

    left_lanes = lax.broadcasted_iota(jnp.int32, (256, 128), 1) < 64

    def multiply(i):
        block, slot = pl.ds(i * 256, 256), slots[i]

        def arrive(a):
            @pl.when(k == i % 2)
            def _():
                wait(full.at[a, block], d_sem.at[i, a])

        arrive(0)
        acc[slot, :, 0:1024] = dot_t(full[0, block, :], w_gu[...])
        arrive(1)
        acc[slot, :, 1024:1536] = dot_t(full[1, block, :], w_b[...])
        both = acc[slot, :, 1408:1536]
        acc[slot, :, 896:1024] = jnp.where(left_lanes | (k == 1), both, acc[slot, :, 896:1024])

    xp, xm = off(x, 1, NX), off(x, 3, NX)
    sends = []

    def x_send(src, dst, rsem, to):
        c = remote(src, dst, xs_sem.at[len(sends)], rsem, dev(to, y, z, k))
        c.start()
        sends.append(c)

    def x_put(i, h, dst, rsem, to, plus=None):
        part = pl.ds(h * 128, 128)
        v = acc[slots[i], part, 0:1408]
        if plus is not None:
            v = v + decoded(plus)
        enc[i, part] = encoded(v)
        x_send(enc.at[i, part], dst, rsem, to)

    top, low = pl.ds(0, 128), pl.ds(128, 128)

    def x_step(i):
        if i == 0:
            x_put(0, 0, rh.at[0], rh_sem.at[0], xp)
            x_put(0, 1, rh.at[1], rh_sem.at[1], xm)
        elif i == 1:
            x_put(1, 0, rx.at[1, top], rx_sem.at[1, 0], xm)
            x_put(1, 1, rx.at[0, low], rx_sem.at[0, 1], xp)
        else:
            wait(rh.at[0], rh_sem.at[0])
            x_put(2, 0, rx.at[0, top], rx_sem.at[0, 0], xp, rh[0])
            wait(rh.at[1], rh_sem.at[1])
            x_put(2, 1, rx.at[1, low], rx_sem.at[1, 1], xm, rh[1])

    steps = {"a1": functools.partial(a_step, 1)}
    for n in range(2):
        for q in range(5):
            steps["z%d_%d" % (n, q)] = functools.partial(z_step, n, q)
        steps["y%dn" % n] = functools.partial(y_step, n, 1)
        steps["y%ds" % n] = functools.partial(y_step, n, 0)
    for i in range(4):
        steps["m%d" % i] = functools.partial(multiply, i)
    for i in range(3):
        steps["x%d" % i] = functools.partial(x_step, i)
    for name in SCHEDULE:
        if name == "m0":
            for c in loads:
                c.wait()
        with jax.named_scope(name):
            steps[name]()

    for n, s in ((1, 0), (0, 1), (0, 0), (1, 1)):
        part = pl.ds(s * 128, 128)
        wait(rx.at[n, part], rx_sem.at[n, s])
        acc[0, part, 0:1408] = acc[0, part, 0:1408] + decoded(rx[n, part])
    ml[0] = acc[0, :, 896:1024]
    model = remote(ml.at[0], ml.at[1], ml_sem.at[0], ml_sem.at[1], dev(x, y, z, sib))
    model.start()

    lane = lax.broadcasted_iota(jnp.int32, (32, 128), 1) < 64
    projected = []
    for s in range(2):
        part = pl.ds(s * 128, 128)
        gg, gu, hid = layer(acc[0, part, 0:384], acc[0, part, 384:768], acc[0, part, 1024:1408])
        left = acc[0, part, 768:896]
        ggl, gul, hil = layer(left, pltpu.roll(left, 64, 1), acc[0, part, 896:1024])
        pgu = dot_t(gg, hpz[64:192, 0:384]) + dot_t(ggl[:, 0:64], hpz[64:192, 384:448])
        pgu += dot_t(gu, hpz[0:128, 0:384]) + dot_t(gul[:, 0:64], hpz[0:128, 384:448])
        ph = dot_t(hid, hpz[64:192, 0:384]) + dot_t(hil[:, 0:64], hpz[64:192, 384:448])
        projected.append((pgu, ph))
    model.wait()
    for s in range(2):
        part = pl.ds(s * 128, 128)
        pgu, ph = projected[s]
        mine, other = ml[0, part], ml[1, part]
        m_tok = jnp.where(k == 0, mine, other)
        m_cot = jnp.where(k == 0, other, mine)
        g_tmp[0] = exact_dot(m_tok.T, pgu)
        g_tmp[1] = exact_dot(ph.T, m_cot)
        even, odd = g_tmp[0, pl.ds(64, 32, 2), :], g_tmp[0, pl.ds(65, 32, 2), :]
        gpart[s, 0:32] = jnp.where(lane, even, pltpu.roll(odd, 64, 1))
        gpart[s, 32:64] = jnp.where(lane, pltpu.roll(even, 64, 1), odd)
        even, odd = g_tmp[1, pl.ds(0, 32, 2), :], g_tmp[1, pl.ds(1, 32, 2), :]
        gpart[s, 64:96] = jnp.where(lane, pltpu.roll(even, 64, 1), odd)

    def share(q):
        return pl.ds(pl.multiple_of(q * 24, 8), 24)

    near = [(oy, ok) for oy in range(NY) for ok in range(2) if oy or ok]
    for n, (oy, ok) in enumerate(near):
        y_, k_ = off(y, oy, NY), off(k, ok, 2)
        remote(gpart.at[k_, share(y_)], r8.at[n], snd_sem.at[7], r8_sem.at[n], dev(x, y_, z, k_)).start()
    total = gpart[k, share(y)]
    for n in range(7):
        wait(r8.at[n], r8_sem.at[n])
        total += r8[n]
    s24[...] = total
    for n in range(7):
        remote(s24, rz.at[n], snd_sem.at[8], rz_sem.at[n], dev(x, y, off(z, n + 1, NZ), k)).start()
    for n in range(7):
        wait(rz.at[n], rz_sem.at[n])
        total += rz[n]
    gs[k, share(y)] = total
    for n, (oy, ok) in enumerate(near):
        y_, k_ = off(y, oy, NY), off(k, ok, 2)
        ref = gs.at[k, share(y)]
        remote(ref, ref, snd_sem.at[9], gs_sem.at[n], dev(x, y_, z, k_)).start()
    for n in range(7):
        wait(r8.at[n], gs_sem.at[n])

    sums = [jnp.zeros((16, 128), F32), jnp.zeros((16, 128), F32)]
    for p in range(96):
        q = qv[:, p * 128 : (p + 1) * 128].astype(F32)
        for s in range(2):
            sums[s] += q * gs[s, p : p + 1, :]
    for s in range(2):
        out[s, :] = sums[s].sum(1)

    for _, c, here, slot, _ in a_sends:

        @pl.when((lax.rem(slot, 2) == 1 - k) & jnp.logical_not(here))
        def _(c=c):
            c.wait_send()

    wait(full.at[0, pl.ds(0, 448)], snd_sem.at[0])
    wait(full.at[0, pl.ds(0, 512)], snd_sem.at[1])
    wait(full.at[0], snd_sem.at[2])
    for c in sends:
        c.wait_send()
    for n in (7, 8, 9):
        wait(r8, snd_sem.at[n])


def on_device(tok, cot, wg, wu, wd, mp, hp, qs):
    depth = wg.shape[0]
    wg, wu = wg.T, wu.T
    any_ = pl.BlockSpec(memory_space=pl.ANY)
    dma = pltpu.SemaphoreType.DMA
    return pl.pallas_call(
        kernel,
        out_shape=jax.ShapeDtypeStruct((2, 16), F32),
        in_specs=[any_] * 8,
        out_specs=pl.BlockSpec(memory_space=pltpu.VMEM),
        scratch_shapes=[
            pltpu.VMEM((2, 256, 512), BF16),
            pltpu.VMEM((2, 1024, depth), BF16),
            pltpu.VMEM((1024, depth), BF16),
            pltpu.VMEM((512, depth), BF16),
            pltpu.VMEM((192, 448), BF16),
            pltpu.VMEM((16, 12288), BF16),
            pltpu.VMEM((3, 256, 1408), BF16),
            pltpu.VMEM((2, 128, 1408), BF16),
            pltpu.VMEM((2, 256, 1408), BF16),
            pltpu.VMEM((3, 256, 1536), F32),
            pltpu.VMEM((2, 256, 128), F32),
            pltpu.VMEM((2, 128, 128), F32),
            pltpu.VMEM((2, 96, 128), F32),
            pltpu.VMEM((7, 24, 128), F32),
            pltpu.VMEM((24, 128), F32),
            pltpu.VMEM((7, 24, 128), F32),
            pltpu.VMEM((2, 96, 128), F32),
            dma((11,)),
            dma((4, 4)),
            dma((2, 4, 4, 4)),
            dma((4, 2)),
            dma((4, 2)),
            dma((10,)),
            dma((4, 4)),
            dma((6,)),
            dma((2,)),
            dma((2, 2)),
            dma((2,)),
            dma((7,)),
            dma((7,)),
            dma((7,)),
        ],
        compiler_params=pltpu.CompilerParams(
            collective_id=0, has_side_effects=True, vmem_limit_bytes=60 * 2**20
        ),
        name="grads_and_scores",
    )(tok, cot, wg, wu, wd, mp, hp, qs).T


def solution(mesh):
    return jax.shard_map(
        on_device,
        mesh=mesh,
        in_specs=(
            P("fsdp", "dp"),
            P("fsdp", "dp"),
            P("fsdp", ("tensor", "dp")),
            P("fsdp", ("tensor", "dp")),
            P(("tensor", "dp"), "fsdp"),
            P(),
            P(None, ("tensor", "dp")),
            P("dp", None),
        ),
        out_specs=P("dp", "fsdp"),
        check_vma=False,
    )
```
